32 devices in a mesh: copy: 4 (over z), row: 4 (over x, core), col: 2 (over y).
Axes of the slice: x: 2, y: 2, z: 4, core: 2. Of those that a mesh axis runs over, the one named last changes fastest.
Arguments:
- trailing: float32 [32768, 16, 2, 128], P(('copy', 'row'), None, 'col'), parts along dimension 0, may hold values from -6 to 6
- lower_trail: float32 [64, 2, 128, 768], P(('copy', 'row'), None, None, 'col'), parts along dimension 0, may hold values from -0.09375 to 0.09375
- lower_cross: float32 [384, 384], replicated, may hold values from -0.3125 to 0.3125
- panel_inverse: float32 [2, 384, 384], replicated, may hold values from -1 to 1, as said below
- target: float32 [32768, 2, 384], P(('copy', 'row'), None, 'col'), parts along dimension 0, may hold values from -6 to 6
Outputs:
- inverse_panels: float32 [32768, 2, 384], P(('copy', 'row'), None, 'col'), parts along dimension 0
The draws below stay inside these ranges and needn't reach their ends.
There are 4 independent parts, one for each index of `copy`. The reference program is written for one: setup_inputs(seed, part) draws one part's arguments, and reference() takes and returns one part's arrays. A program takes and returns all parts, laid end to end along the dimension named above; an argument that names none is the same for every part. Nothing has to cross between parts.
Inputs may be any that keep to these rules, and one draw needn't show every extreme that they name: `panel_inverse`: each of the two 384 x 384 matrices is unit lower triangular: ones on the diagonal, zeros above it.
All inputs are finite; a program needn't handle non-finite values.
Results may differ from the reference program's by a relative error of at most 0.000071.
Values sent between devices are 32-bit elements; how exact they have to be, the bound alone decides.
A program may use at most 192 MiB of HBM per device.

```python
import jax
import jax.numpy as jnp
from jax import lax

PW = 384
NB = 128
TQ = 16
ROWS = 8192
TRAIL = 4096
N_COL = 2


def draw_panel_inverse(key, part):
    strict_lower = jnp.tril(jnp.ones((PW, PW), jnp.float32), -1)
    values = jax.random.normal(key, (2, PW, PW), jnp.float32) / PW ** 0.5
    values = jnp.clip(values, -1.0, 1.0)
    return values * strict_lower + jnp.eye(PW, dtype=jnp.float32)


def block_scale(rng, shape, pieces, low, high):
    def one(dim, parts):
        draws = jax.random.uniform(jax.random.fold_in(jax.random.fold_in(rng, 6), dim), (parts,), jnp.float32, low / len(pieces), high / len(pieces))
        return jnp.repeat(jnp.exp(draws), shape[dim] // parts).reshape((-1,) + (1,) * (len(shape) - dim - 1))

    loudness = one(*pieces[0])
    for cut in pieces[1:]:
        loudness = loudness * one(*cut)
    return loudness


def normal_values(key, dims, deviation, reach, split=(), kind=jnp.bfloat16):
    array = deviation * jax.random.normal(key, dims, jnp.float32)
    if split:
        array = array * block_scale(key, dims, split, -0.22, 0.18)
    return jnp.clip(array, -reach, reach).astype(kind)


def setup_inputs(seed: int = 0, part: int = 0) -> dict:
    arg_keys = jax.random.split(jax.random.key(seed), 6)
    own_keys = jax.random.split(jax.random.fold_in(arg_keys[5], part), 6)
    return {
        "trailing": normal_values(own_keys[0], (ROWS, TQ, N_COL, NB), 1.0, 6.0, ((0, 4), (2, 2)), jnp.float32),
        "lower_trail": normal_values(own_keys[1], (TQ, N_COL, NB, 2 * PW), TRAIL ** -0.5, 0.09375, ((0, 4), (3, 2)), jnp.float32),
        "lower_cross": normal_values(arg_keys[2], (PW, PW), PW ** -0.5, 0.3125, (), jnp.float32),
        "panel_inverse": draw_panel_inverse(jax.random.fold_in(arg_keys[5], 71), part),
        "target": normal_values(own_keys[4], (ROWS, 2, PW), 1.0, 6.0, ((0, 4), (2, 2)), jnp.float32),
    }


precise = lax.Precision.HIGHEST


def matmul(first, second):
    return jnp.dot(first, second, preferred_element_type=jnp.float32, precision=precise)


def reference(trailing, lower_trail, lower_cross, panel_inverse, target):
    row_count = trailing.shape[0]
    trail_flat = trailing.reshape(row_count, trailing.shape[1] * trailing.shape[2] * trailing.shape[3])
    lower_flat = lower_trail.reshape(trail_flat.shape[1], lower_trail.shape[3])
    update = matmul(trail_flat, lower_flat)
    panel_cols = lower_flat.shape[1] // 2
    right_panel = matmul(target[:, 1, :] - update[:, panel_cols:], panel_inverse[1])
    left_panel = matmul(target[:, 0, :] - update[:, :panel_cols] - matmul(right_panel, lower_cross), panel_inverse[0])
    return jnp.stack([left_panel, right_panel], axis=1)
```

```python
import jax
import jax.numpy as jnp
from jax import lax
from jax.sharding import PartitionSpec as P

CHUNKS = 4


def matmul(first, second, precision=lax.Precision.HIGH):
    return jnp.dot(first, second, preferred_element_type=jnp.float32, precision=precision)


def folded_map(lower_cross, panel_inverse):
    exact = lax.Precision.HIGHEST
    left, right = panel_inverse[0], panel_inverse[1]
    cross = matmul(matmul(right, lower_cross, exact), left, exact)
    top = jnp.concatenate([left, jnp.zeros_like(left)], axis=1)
    bottom = jnp.concatenate([-cross, right], axis=1)
    return jnp.concatenate([top, bottom], axis=0)


def per_device(trailing, lower_trail, lower_cross, panel_inverse, target):
    cols = lax.axis_size("col")
    me = lax.axis_index("col")
    rows, blocks, _, width = trailing.shape
    own_blocks = lower_trail.shape[0]
    depth = own_blocks * width
    panel = lower_cross.shape[0]
    span = 2 * panel
    share = panel // cols
    held = span // cols

    def shift(array, step):
        if cols == 1 or step == 0:
            return array
        return lax.ppermute(array, "col", [(i, (i + step) % cols) for i in range(cols)])

    fold = folded_map(lower_cross, panel_inverse)
    by_owner = fold.reshape(span, 2, cols, share)
    by_owner = jnp.swapaxes(by_owner, 1, 2).reshape(span, cols, 2 * share)

    def owner_cols(matrix, owner):
        return lax.dynamic_index_in_dim(matrix, owner, 1, keepdims=False)

    pieces = []
    for step in range(cols):
        block = lax.dynamic_index_in_dim(lower_trail, (me + step) % cols, 1, keepdims=False)
        pieces.append(shift(block, step).reshape(depth, held))

    trail_flat = trailing.reshape(rows, blocks * width)
    own_target = target.reshape(rows, 2 * share)
    by_owner_rows = by_owner.reshape(2, cols, share, cols, 2 * share)
    own_rows = lax.dynamic_index_in_dim(by_owner_rows, me, 1, keepdims=False)
    own_rows = own_rows.reshape(2 * share, cols, 2 * share)
    held_rows = by_owner.reshape(cols, held, cols, 2 * share)

    gathered = {}
    for step in list(range(1, cols)) + [0]:
        owner = (me + step) % cols
        total = None
        for back, piece in enumerate(pieces):
            source = (me - back) % cols
            weights = lax.dynamic_index_in_dim(held_rows, source, 0, keepdims=False)
            term = matmul(piece, owner_cols(weights, owner))
            total = term if total is None else total + term
        gathered[step] = lax.all_gather(total, "row", axis=0, tiled=True)

    size = rows // CHUNKS
    arrived = [[] for _ in range(CHUNKS)]
    for step in range(1, cols):
        owner = (me + step) % cols
        weights = owner_cols(own_rows, owner)
        for chunk in range(CHUNKS):
            part = slice(chunk * size, (chunk + 1) * size)
            partial = matmul(own_target[part], weights) - matmul(trail_flat[part], gathered[step])
            arrived[chunk].append(shift(partial, step))
    own = matmul(own_target, owner_cols(own_rows, me)) - matmul(trail_flat, gathered[0])
    result = []
    for chunk in range(CHUNKS):
        total = own[chunk * size:(chunk + 1) * size]
        for other in arrived[chunk]:
            total = total + other
        result.append(total)
    return jnp.concatenate(result, axis=0).reshape(rows, 2, share)


def solution(mesh):
    placed = (
        P(("copy", "row"), None, "col", None),
        P(("copy", "row"), None, None, "col"),
        P(),
        P(),
        P(("copy", "row"), None, "col"),
    )
    return jax.shard_map(
        per_device,
        mesh=mesh,
        in_specs=placed,
        out_specs=P(("copy", "row"), None, "col"),
        check_vma=False,
    )
```

```python
import jax
import jax.numpy as jnp
from jax import lax
from jax.experimental import pallas as pl
from jax.experimental.pallas import tpu as pltpu
from jax.sharding import PartitionSpec as P

ROW_TILE = 256
LANES = 128
CHUNKS = 2
exact = lax.Precision.HIGHEST


def matmul(first, second, precision=lax.Precision.HIGH):
    return jnp.dot(first, second, preferred_element_type=jnp.float32, precision=precision)


def contract_last(first, second, precision=lax.Precision.HIGH):
    return lax.dot_general(
        first, second, (((1,), (1,)), ((), ())), preferred_element_type=jnp.float32, precision=precision
    )


def halves(value):
    high = value.astype(jnp.bfloat16)
    return high, (value - high.astype(jnp.float32)).astype(jnp.bfloat16)


def three_pass(first, second):
    first_high, first_low = first
    second_high, second_low = second

    def product(a, b):
        return jnp.dot(a, b, preferred_element_type=jnp.float32)

    return product(first_high, second_high) + (product(first_high, second_low) + product(first_low, second_high))


def share_kernel(trail_ref, factor_ref, weight_ref, target_ref, out_ref, high_ref, low_ref):
    @pl.when(pl.program_id(0) == 0)
    def _():
        high_ref[...], low_ref[...] = halves(factor_ref[...])

    blocks = trail_ref.shape[1]
    trail = jnp.concatenate([trail_ref[:, block, :] for block in range(blocks)], axis=1)
    summed = three_pass(halves(trail), (high_ref[...], low_ref[...]))
    start = three_pass(halves(weight_ref[...]), halves(target_ref[...]))
    out_ref[...] = start - summed.T


def share_of(trail, factor, weight, target, chunk=0, chunks=1):
    rows, blocks, width = trail.shape
    depth, out_cols = factor.shape
    in_cols = target.shape[0]
    count = rows // chunks
    tile = min(ROW_TILE, count)
    begin = chunk * (count // tile)
    return pl.pallas_call(
        share_kernel,
        grid=(count // tile,),
        in_specs=[
            pl.BlockSpec((tile, blocks, width), lambda i: (i + begin, 0, 0)),
            pl.BlockSpec((depth, out_cols), lambda i: (0, 0)),
            pl.BlockSpec((out_cols, in_cols), lambda i: (0, 0)),
            pl.BlockSpec((in_cols, tile), lambda i: (0, i + begin)),
        ],
        out_specs=pl.BlockSpec((out_cols, tile), lambda i: (0, i)),
        out_shape=jax.ShapeDtypeStruct((out_cols, count), jnp.float32),
        scratch_shapes=[pltpu.VMEM((depth, out_cols), jnp.bfloat16)] * 2,
        compiler_params=pltpu.CompilerParams(dimension_semantics=("arbitrary",)),
        cost_estimate=pl.CostEstimate(
            flops=6 * count * depth * out_cols, bytes_accessed=4 * count * depth, transcendentals=0
        ),
    )(trail, factor, weight, target)


def per_device(trailing, lower_trail, lower_cross, panel_inverse, target):
    cols = lax.axis_size("col")
    me = lax.axis_index("col")
    rows, blocks, _, width = trailing.shape
    depth = lower_trail.shape[0] * width
    panel = lower_cross.shape[0]
    span = 2 * panel
    share = panel // cols
    out_cols = 2 * share
    held = span // cols

    def shift(array, step):
        if step == 0:
            return array
        return lax.ppermute(array, "col", [(i, (i + step) % cols) for i in range(cols)])

    pieces = []
    for step in range(cols):
        block = lax.dynamic_index_in_dim(lower_trail, (me + step) % cols, 1, keepdims=False)
        pieces.append(shift(block, step).reshape(depth, held))

    left, right = panel_inverse[0], panel_inverse[1]
    cross = matmul(matmul(right, lower_cross, exact), left, exact)
    top = jnp.concatenate([left.T, -cross.T], axis=1)
    bottom = jnp.concatenate([jnp.zeros_like(left), right.T], axis=1)
    by_owner = jnp.stack([top, bottom]).reshape(2, cols, share, span)

    def owner_fold(owner):
        return lax.dynamic_index_in_dim(by_owner, owner, 1, keepdims=False).reshape(out_cols, span)

    def gathered(fold, part):
        total = None
        for back, piece in enumerate(pieces):
            source = (me - back) % cols
            weights = lax.dynamic_slice_in_dim(fold[part], source * held, held, 1)
            term = contract_last(piece, weights)
            total = term if total is None else total + term
        return lax.all_gather(total, "row", axis=0, tiled=True)

    held_col = jnp.arange(out_cols)
    place = (held_col // share) * panel + me * share + held_col % share
    pick = (place[:, None] == jnp.arange(span)[None, :]).astype(jnp.float32)

    trail = trailing.reshape(rows, blocks, width)
    own_target = target.transpose(1, 2, 0).reshape(out_cols, rows)
    first = LANES if out_cols > LANES else out_cols
    parts = [slice(0, first)] + ([slice(first, out_cols)] if first < out_cols else [])
    folds = [owner_fold((me + step) % cols) for step in range(cols)]
    factors = {}
    for step in range(1, cols):
        for index, part in enumerate(parts):
            factors[step, index] = gathered(folds[step], part)
    own_factor = gathered(folds[0], slice(0, out_cols))

    chunks = CHUNKS if rows % (CHUNKS * LANES) == 0 else 1
    arrived = [[[] for _ in range(chunks)] for _ in parts]
    for step in range(1, cols):
        weights = contract_last(folds[step], pick, exact)
        for index, part in enumerate(parts):
            for chunk in range(chunks):
                partial = share_of(trail, factors[step, index], weights[part], own_target, chunk, chunks)
                arrived[index][chunk].append(shift(partial, step))
    own = share_of(trail, own_factor, contract_last(folds[0], pick, exact), own_target)
    if cols == 1:
        return own.reshape(2, share, rows).transpose(2, 0, 1)
    others = []
    for pieces_here in arrived:
        sums = [sum(group[1:], group[0]) for group in pieces_here]
        others.append(jnp.concatenate(sums, axis=1))
    result = own + jnp.concatenate(others, axis=0)
    return result.reshape(2, share, rows).transpose(2, 0, 1)


def solution(mesh):
    placed = (
        P(("copy", "row"), None, "col", None),
        P(("copy", "row"), None, None, "col"),
        P(),
        P(),
        P(("copy", "row"), None, "col"),
    )
    return jax.shard_map(
        per_device,
        mesh=mesh,
        in_specs=placed,
        out_specs=P(("copy", "row"), None, "col"),
        check_vma=False,
    )
```
